512 devices in a mesh: gx: 64 (over z_hi, y, core), gy: 8 (over z_lo, x).
Axes of the slice: x: 4, y: 8, z: 8 (z_hi: 4, z_lo: 2; z = z_hi * 2 + z_lo), core: 2. Of those that a mesh axis runs over, the one named last changes fastest.
Arguments:
- field: bfloat16 [1, 512, 512, 128], P(None, 'gx', 'gy'), may hold values from -6 to 6
- conv_weight: bfloat16 [3, 3, 128, 128], replicated, may hold values from -0.1875 to 0.1875
- qkv_weight: bfloat16 [128, 384], replicated, may hold values from -4 to 4
- out_weight: bfloat16 [128, 128], replicated, may hold values from -0.5 to 0.5
Outputs:
- result: bfloat16 [1, 512, 512, 128], P(None, 'gx', 'gy')
The draws below stay inside these ranges and needn't reach their ends.
All inputs are finite; a program needn't handle non-finite values.
Results may differ from the reference program's by a relative error of at most 0.0064.
Values may be sent and summed in bfloat16 or wider, within the bound.
No kernel may reach another device: no remote copies, remote signals or barrier semaphores. Data moves between devices by JAX's collectives and lax.ppermute only.
A program may use at most 64 MiB of HBM per device.

```python
import jax
import jax.numpy as jnp
from jax import lax

C = 128
HEADS = 4
HEAD = 32
Z = 1
NX = 512
NY = 512


def draw_qkv_weight(key, part):
    keys = jax.random.split(key, 1)
    scale = C ** (-0.5)
    base = jnp.clip(jax.random.normal(keys[0], (C, 3 * C), jnp.float32), -4.0, 4.0) * scale
    return base.astype(jnp.bfloat16)


def block_levels(rng, dims, cuts, smallest, top_value):
    factor_of = 1.0
    for position, shards_of in cuts:
        draws = jax.random.uniform(jax.random.fold_in(jax.random.fold_in(rng, 6), position), (shards_of,), jnp.float32, smallest / len(cuts), top_value / len(cuts))
        factor_of = factor_of * jnp.repeat(jnp.exp(draws), dims[position] // shards_of).reshape((-1,) + (1,) * (len(dims) - 1 - position))
    return factor_of


def normal_values(rng, extent, deviation, limit, shards=(), held_as=jnp.bfloat16):
    level = block_levels(rng, extent, shards, -0.22, 0.18) if shards else 1.0
    entries = jax.random.normal(rng, extent, jnp.float32) * deviation * level
    return jnp.minimum(jnp.maximum(entries, -limit), limit).astype(held_as)


def setup_inputs(seed: int = 0) -> dict:
    key_list = jax.random.split(jax.random.key(seed), 5)
    return {
        "field": normal_values(key_list[0], (Z, NX, NY, C), 1.0, 6.0, ((1, 64), (2, 8))),
        "conv_weight": normal_values(key_list[1], (3, 3, C, C), (9 * C) ** -0.5, 0.1875),
        "qkv_weight": draw_qkv_weight(jax.random.fold_in(key_list[4], 71), 0),
        "out_weight": normal_values(key_list[3], (C, C), C ** -0.5, 0.5),
    }


def stem_conv(field, conv_weight):
    total = jnp.zeros(field.shape, jnp.float32)
    for a in range(3):
        for b in range(3):
            moved = jnp.roll(field, (1 - a, 1 - b), axis=(1, 2))
            part = jnp.dot(moved.reshape(-1, C), conv_weight[a, b], preferred_element_type=jnp.float32)
            total = total + part.reshape(field.shape)
    return total

def attend_line(column):
    query = column[:, :C].reshape(NX, HEADS, HEAD).astype(jnp.float32)
    keyed = column[:, C:2 * C].reshape(NX, HEADS, HEAD).astype(jnp.float32)
    valued = column[:, 2 * C:].reshape(NX, HEADS, HEAD).astype(jnp.float32)
    scores = jnp.einsum('qhd,khd->hqk', query, keyed) / jnp.sqrt(jnp.float32(HEAD))
    top = lax.optimization_barrier(jnp.max(scores, axis=-1, keepdims=True))
    expo = jnp.exp(scores - top)
    probs = (expo / lax.optimization_barrier(jnp.sum(expo, axis=-1, keepdims=True))).astype(jnp.bfloat16)
    mixed = jnp.einsum('hqk,khd->qhd', probs.astype(jnp.float32), valued)
    return mixed.reshape(NX, C).astype(jnp.bfloat16)

def reference(field, conv_weight, qkv_weight, out_weight):
    stem = stem_conv(field, conv_weight)
    mean = lax.optimization_barrier(jnp.mean(stem, axis=-1, keepdims=True))
    varia = lax.optimization_barrier(jnp.mean((stem - mean) ** 2, axis=-1, keepdims=True))
    normed = ((stem - mean) / jnp.sqrt(varia + 1e-05)).astype(jnp.bfloat16)
    qkv = jnp.dot(normed.reshape(-1, C), qkv_weight, preferred_element_type=jnp.float32).astype(jnp.bfloat16)
    qkv = qkv.reshape(Z, NX, NY, 3 * C)
    columns = jnp.transpose(qkv, (0, 2, 1, 3)).reshape(Z * NY, NX, 3 * C)
    attended = lax.map(attend_line, columns)
    attended = jnp.transpose(attended.reshape(Z, NY, NX, C), (0, 2, 1, 3))
    projected = jnp.dot(attended.reshape(-1, C), out_weight, preferred_element_type=jnp.float32)
    return (stem + projected.reshape(stem.shape)).astype(jnp.bfloat16)
```

```python
import jax
import jax.numpy as jnp
from jax import lax
from jax.sharding import PartitionSpec as P

HEADS = 4
HEAD = 32


def to_lines(block):
    return lax.all_to_all(block, "gx", split_axis=2, concat_axis=1, tiled=True)


def to_blocks(lines):
    return lax.all_to_all(lines, "gx", split_axis=1, concat_axis=2, tiled=True)


def neighbour_lines(line):
    n_gx, n_gy = lax.axis_size("gx"), lax.axis_size("gy")
    count = n_gx * n_gy

    def device(c):
        c = c % count
        return (c % n_gx) * n_gy + c // n_gx

    from_left = lax.ppermute(line, ("gx", "gy"), [(device(c), device(c + 1)) for c in range(count)])
    from_right = lax.ppermute(line, ("gx", "gy"), [(device(c + 1), device(c)) for c in range(count)])
    return from_left, from_right


def convolve(columns, conv_weight):
    length, width = columns.shape[1], columns.shape[2]
    taps = []
    for a in range(3):
        for b in range(3):
            taps.append(jnp.roll(columns[b], 1 - a, axis=0))
    stacked = jnp.concatenate(taps, axis=1)
    return jnp.dot(
        stacked, conv_weight.reshape(9 * width, width), preferred_element_type=jnp.float32
    )


def normalize(stem):
    mean = jnp.mean(stem, axis=-1, keepdims=True)
    varia = jnp.mean((stem - mean) ** 2, axis=-1, keepdims=True)
    return ((stem - mean) / jnp.sqrt(varia + 1e-05)).astype(jnp.bfloat16)


def attend(normed, qkv_weight):
    length, width = normed.shape
    qkv = jnp.dot(normed, qkv_weight, preferred_element_type=jnp.float32).astype(jnp.bfloat16)
    query = qkv[:, :width].reshape(length, HEADS, HEAD)
    keyed = qkv[:, width : 2 * width].reshape(length, HEADS, HEAD)
    valued = qkv[:, 2 * width :].reshape(length, HEADS, HEAD)
    scores = jnp.einsum("qhd,khd->hqk", query, keyed, preferred_element_type=jnp.float32)
    scores = scores / jnp.sqrt(jnp.float32(HEAD))
    top = jnp.max(scores, axis=-1, keepdims=True)
    expo = jnp.exp(scores - top)
    probs = (expo / jnp.sum(expo, axis=-1, keepdims=True)).astype(jnp.bfloat16)
    mixed = jnp.einsum("hqk,khd->qhd", probs, valued, preferred_element_type=jnp.float32)
    return mixed.astype(jnp.bfloat16).reshape(length, width)


def on_device(field, conv_weight, qkv_weight, out_weight):
    lines = to_lines(field)
    planes, length, _, width = lines.shape
    line = lines.reshape(length, width)
    from_left, from_right = neighbour_lines(line)
    stem = convolve(jnp.stack([from_left, line, from_right]), conv_weight)
    normed = normalize(stem)
    attended = attend(normed, qkv_weight)
    projected = jnp.dot(attended, out_weight, preferred_element_type=jnp.float32)
    result = (stem + projected).astype(jnp.bfloat16)
    return to_blocks(result.reshape(planes, length, 1, width))


def solution(mesh):
    placed = (P(None, "gx", "gy", None), P(), P(), P())
    return jax.shard_map(
        on_device, mesh=mesh, in_specs=placed, out_specs=P(None, "gx", "gy", None), check_vma=False
    )
```

```python
import jax
import jax.numpy as jnp
from jax import lax
from jax.sharding import PartitionSpec as P

HEADS = 4
HEAD = 32


def padded_columns(block):
    count = lax.axis_size("gy")
    left = lax.ppermute(block[:, :, -1:], "gy", [(i, (i + 1) % count) for i in range(count)])
    right = lax.ppermute(block[:, :, :1], "gy", [((i + 1) % count, i) for i in range(count)])
    return jnp.concatenate([left, block, right], axis=2)


def to_lines(padded):
    cols = padded.shape[2] - 2
    windows = jnp.stack([padded[:, :, b : b + cols] for b in range(3)], axis=3)
    return lax.all_to_all(windows, "gx", split_axis=2, concat_axis=1, tiled=True)


def to_blocks(lines):
    return lax.all_to_all(lines, "gx", split_axis=1, concat_axis=2, tiled=True)


def convolve(columns, conv_weight):
    length, width = columns.shape[1], columns.shape[2]
    taps = []
    for a in range(3):
        for b in range(3):
            taps.append(jnp.roll(columns[b], 1 - a, axis=0))
    stacked = jnp.concatenate(taps, axis=1)
    return jnp.dot(
        stacked, conv_weight.reshape(9 * width, width), preferred_element_type=jnp.float32
    )


def normalize(stem):
    mean = jnp.mean(stem, axis=-1, keepdims=True)
    varia = jnp.mean((stem - mean) ** 2, axis=-1, keepdims=True)
    return ((stem - mean) / jnp.sqrt(varia + 1e-05)).astype(jnp.bfloat16)


def attend(normed, qkv_weight):
    length, width = normed.shape
    qkv = jnp.dot(normed, qkv_weight, preferred_element_type=jnp.float32).astype(jnp.bfloat16)
    query = qkv[:, :width].reshape(length, HEADS, HEAD)
    keyed = qkv[:, width : 2 * width].reshape(length, HEADS, HEAD)
    valued = qkv[:, 2 * width :].reshape(length, HEADS, HEAD)
    scores = jnp.einsum("qhd,khd->hqk", query, keyed, preferred_element_type=jnp.float32)
    scores = scores / jnp.sqrt(jnp.float32(HEAD))
    top = jnp.max(scores, axis=-1, keepdims=True)
    expo = jnp.exp(scores - top)
    probs = (expo / jnp.sum(expo, axis=-1, keepdims=True)).astype(jnp.bfloat16)
    mixed = jnp.einsum("hqk,khd->qhd", probs, valued, preferred_element_type=jnp.float32)
    return mixed.astype(jnp.bfloat16).reshape(length, width)


def on_device(field, conv_weight, qkv_weight, out_weight):
    lines = to_lines(padded_columns(field))
    planes, length, _, _, width = lines.shape
    columns = jnp.moveaxis(lines.reshape(length, 3, width), 1, 0)
    stem = convolve(columns, conv_weight)
    normed = normalize(stem)
    attended = attend(normed, qkv_weight)
    projected = jnp.dot(attended, out_weight, preferred_element_type=jnp.float32)
    result = (stem + projected).astype(jnp.bfloat16)
    return to_blocks(result.reshape(planes, length, 1, width))


def solution(mesh):
    placed = (P(None, "gx", "gy", None), P(), P(), P())
    return jax.shard_map(
        on_device, mesh=mesh, in_specs=placed, out_specs=P(None, "gx", "gy", None), check_vma=False
    )
```

```python
import jax
import jax.numpy as jnp
from jax import lax
from jax.experimental import pallas as pl
from jax.experimental.pallas import tpu as pltpu
from jax.sharding import PartitionSpec as P

HEADS = 4
HEAD = 32


def padded_columns(block):
    count = lax.axis_size("gy")
    left = lax.ppermute(block[:, :, -1:], "gy", [(i, (i + 1) % count) for i in range(count)])
    right = lax.ppermute(block[:, :, :1], "gy", [((i + 1) % count, i) for i in range(count)])
    return jnp.concatenate([left, block, right], axis=2)


def to_lines(padded):
    cols = padded.shape[2] - 2
    windows = jnp.stack([padded[:, :, b : b + cols] for b in range(3)], axis=3)
    return lax.all_to_all(windows, "gx", split_axis=2, concat_axis=1, tiled=True)


def to_blocks(lines):
    return lax.all_to_all(lines, "gx", split_axis=1, concat_axis=2, tiled=True)


def line_kernel(x_ref, cw_ref, qw_ref, ow_ref, o_ref):
    length = x_ref.shape[0]
    width = o_ref.shape[1]
    x = x_ref[...]
    ys = [jnp.dot(x, cw_ref[a], preferred_element_type=jnp.float32) for a in range(3)]
    stem = ys[1] + pltpu.roll(ys[0], 1, 0) + pltpu.roll(ys[2], length - 1, 0)
    mean = jnp.mean(stem, axis=-1, keepdims=True)
    centred = stem - mean
    varia = jnp.mean(centred * centred, axis=-1, keepdims=True)
    normed = (centred / jnp.sqrt(varia + 1e-05)).astype(jnp.bfloat16)
    qkv = jnp.dot(normed, qw_ref[...], preferred_element_type=jnp.float32).astype(jnp.bfloat16)
    scale = 1.0 / jnp.sqrt(jnp.float32(HEAD))
    total = stem
    for h in range(HEADS):
        q = qkv[:, h * HEAD:(h + 1) * HEAD]
        k = qkv[:, width + h * HEAD:width + (h + 1) * HEAD]
        v = qkv[:, 2 * width + h * HEAD:2 * width + (h + 1) * HEAD]
        s = lax.dot_general(q, k, (((1,), (1,)), ((), ())), preferred_element_type=jnp.float32)
        s = s * scale
        m = jnp.max(s, axis=1, keepdims=True)
        e = jnp.exp(s - m)
        l = jnp.sum(e, axis=1, keepdims=True)
        p = (e * (1.0 / l)).astype(jnp.bfloat16)
        o = jnp.dot(p, v, preferred_element_type=jnp.float32).astype(jnp.bfloat16)
        total = total + jnp.dot(o, ow_ref[h * HEAD:(h + 1) * HEAD, :], preferred_element_type=jnp.float32)
    o_ref[...] = total.astype(o_ref.dtype)


def line_block(lines, conv_weight, qkv_weight, out_weight):
    length = lines.shape[0]; width = out_weight.shape[1]
    cw = conv_weight.reshape(3, 3 * width, width)
    vm = pl.BlockSpec(memory_space=pltpu.VMEM)
    return pl.pallas_call(line_kernel, out_shape=jax.ShapeDtypeStruct((length, width), jnp.bfloat16),
        in_specs=[vm]*4, out_specs=vm)(lines, cw, qkv_weight, out_weight)


def on_device(field, conv_weight, qkv_weight, out_weight):
    lines = to_lines(padded_columns(field))
    planes, length, _, taps, width = lines.shape
    result = line_block(lines.reshape(length, taps * width), conv_weight, qkv_weight, out_weight)
    return to_blocks(result.reshape(planes, length, 1, width))


def solution(mesh):
    placed = (P(None, "gx", "gy", None), P(), P(), P())
    return jax.shard_map(
        on_device, mesh=mesh, in_specs=placed, out_specs=P(None, "gx", "gy", None), check_vma=False
    )
```

```python
import jax
import jax.numpy as jnp
from jax import lax
from jax.experimental import pallas as pl
from jax.experimental.pallas import tpu as pltpu
from jax.sharding import PartitionSpec as P

HEADS = 4
HEAD = 32


def padded_columns(block):
    count = lax.axis_size("gy")
    left = lax.ppermute(block[:, :, -1:], "gy", [(i, (i + 1) % count) for i in range(count)])
    right = lax.ppermute(block[:, :, :1], "gy", [((i + 1) % count, i) for i in range(count)])
    return jnp.concatenate([left, block, right], axis=2)


def to_lines(padded):
    cols = padded.shape[2] - 2
    windows = jnp.stack([padded[:, :, b : b + cols] for b in range(3)], axis=3)
    return lax.all_to_all(windows, "gx", split_axis=2, concat_axis=1, tiled=True)


def to_blocks(result, rows):
    length, width = result.shape
    chunks = result.reshape(length // rows, rows, 1, width)
    return lax.all_to_all(chunks, "gx", split_axis=0, concat_axis=2, tiled=True)


def line_kernel(x_ref, cw_ref, qw_ref, ow_ref, o_ref):
    length = x_ref.shape[0]
    width = o_ref.shape[1]
    x = x_ref[...]
    ys = [jnp.dot(x, cw_ref[a], preferred_element_type=jnp.float32) for a in range(3)]
    stem = ys[1] + pltpu.roll(ys[0], 1, 0) + pltpu.roll(ys[2], length - 1, 0)
    mean = jnp.mean(stem, axis=-1, keepdims=True)
    centred = stem - mean
    varia = jnp.mean(centred * centred, axis=-1, keepdims=True)
    normed = (centred / jnp.sqrt(varia + 1e-05)).astype(jnp.bfloat16)
    qkv = jnp.dot(normed, qw_ref[...], preferred_element_type=jnp.float32).astype(jnp.bfloat16)
    scale = 1.0 / jnp.sqrt(jnp.float32(HEAD))
    total = stem
    for h in range(HEADS):
        q = qkv[:, h * HEAD:(h + 1) * HEAD]
        k = qkv[:, width + h * HEAD:width + (h + 1) * HEAD]
        v = qkv[:, 2 * width + h * HEAD:2 * width + (h + 1) * HEAD]
        s = lax.dot_general(q, k, (((1,), (1,)), ((), ())), preferred_element_type=jnp.float32)
        s = s * scale
        m = jnp.max(s, axis=1, keepdims=True)
        e = jnp.exp(s - m)
        l = jnp.sum(e, axis=1, keepdims=True)
        p = (e * (1.0 / l)).astype(jnp.bfloat16)
        o = jnp.dot(p, v, preferred_element_type=jnp.float32).astype(jnp.bfloat16)
        total = total + jnp.dot(o, ow_ref[h * HEAD:(h + 1) * HEAD, :], preferred_element_type=jnp.float32)
    o_ref[...] = total.astype(o_ref.dtype)


def line_block(lines, conv_weight, qkv_weight, out_weight):
    length = lines.shape[0]; width = out_weight.shape[1]
    cw = conv_weight.reshape(3, 3 * width, width)
    vm = pl.BlockSpec(memory_space=pltpu.VMEM)
    return pl.pallas_call(line_kernel, out_shape=jax.ShapeDtypeStruct((length, width), jnp.bfloat16),
        in_specs=[vm]*4, out_specs=vm)(lines, cw, qkv_weight, out_weight)


def on_device(field, conv_weight, qkv_weight, out_weight):
    lines = to_lines(padded_columns(field))
    planes, length, _, taps, width = lines.shape
    result = line_block(lines.reshape(length, taps * width), conv_weight, qkv_weight, out_weight)
    return to_blocks(result, field.shape[1])


def solution(mesh):
    placed = (P(None, "gx", "gy", None), P(), P(), P())
    return jax.shard_map(
        on_device, mesh=mesh, in_specs=placed, out_specs=P(None, "gx", "gy", None), check_vma=False
    )
```

```python
import jax
import jax.numpy as jnp
from jax import lax
from jax.experimental import pallas as pl
from jax.experimental.pallas import tpu as pltpu
from jax.sharding import PartitionSpec as P

HEADS = 4
HEAD = 32


def padded_columns(block):
    count = lax.axis_size("gy")
    left = lax.ppermute(block[:, :, -1:], "gy", [(i, (i + 1) % count) for i in range(count)])
    right = lax.ppermute(block[:, :, :1], "gy", [((i + 1) % count, i) for i in range(count)])
    return jnp.concatenate([left, block, right], axis=2)


def to_lines(padded):
    cols = padded.shape[2] - 2
    windows = jnp.stack([padded[:, :, b : b + cols] for b in range(3)], axis=3)
    return lax.all_to_all(windows, "gx", split_axis=2, concat_axis=1, tiled=True)


def to_blocks(result, rows):
    length, width = result.shape
    chunks = result.reshape(length // rows, rows, 1, width)
    return lax.all_to_all(chunks, "gx", split_axis=0, concat_axis=2, tiled=True)


def line_kernel(x_ref, cw_ref, qw_ref, ow_ref, o_ref):
    length = x_ref.shape[0]
    width = o_ref.shape[1]
    x = x_ref[...]
    taps = jnp.dot(x, jnp.concatenate([cw_ref[a] for a in range(3)], axis=1),
                   preferred_element_type=jnp.float32)
    stem = (taps[:, width:2 * width] + pltpu.roll(taps[:, :width], 1, 0)
            + pltpu.roll(taps[:, 2 * width:], length - 1, 0))
    mean = jnp.mean(stem, axis=-1, keepdims=True)
    centred = stem - mean
    varia = jnp.mean(centred * centred, axis=-1, keepdims=True)
    normed = (centred / jnp.sqrt(varia + 1e-05)).astype(jnp.bfloat16)
    qkv = jnp.dot(normed, qw_ref[...], preferred_element_type=jnp.float32).astype(jnp.bfloat16)
    query, keyed, valued = qkv[:, :width], qkv[:, width:2 * width], qkv[:, 2 * width:]
    head_of = lax.broadcasted_iota(jnp.int32, (length, width), 1) // HEAD
    zero = jnp.zeros_like(keyed)
    keys = jnp.concatenate([jnp.where(head_of == h, keyed, zero) for h in range(HEADS)], axis=0)
    values = jnp.concatenate([jnp.where(head_of == h, valued, zero) for h in range(HEADS)], axis=0)
    scores = lax.dot_general(query, keys, (((1,), (1,)), ((), ())), preferred_element_type=jnp.float32)
    scale = 1.0 / jnp.sqrt(jnp.float32(HEAD))
    weights, inverse = [], jnp.zeros((length, width), jnp.float32)
    for h in range(HEADS):
        s = scores[:, h * length:(h + 1) * length] * scale
        e = jnp.exp(s - jnp.max(s, axis=1, keepdims=True))
        weights.append(e.astype(jnp.bfloat16))
        inverse = jnp.where(head_of == h, 1.0 / jnp.sum(e, axis=1, keepdims=True), inverse)
    mixed = jnp.dot(jnp.concatenate(weights, axis=1), values, preferred_element_type=jnp.float32)
    attended = (mixed * inverse).astype(jnp.bfloat16)
    total = stem + jnp.dot(attended, ow_ref[...], preferred_element_type=jnp.float32)
    o_ref[...] = total.astype(o_ref.dtype)


def line_block(lines, conv_weight, qkv_weight, out_weight):
    length = lines.shape[0]; width = out_weight.shape[1]
    cw = conv_weight.reshape(3, 3 * width, width)
    vm = pl.BlockSpec(memory_space=pltpu.VMEM)
    return pl.pallas_call(line_kernel, out_shape=jax.ShapeDtypeStruct((length, width), jnp.bfloat16),
        in_specs=[vm]*4, out_specs=vm)(lines, cw, qkv_weight, out_weight)


def on_device(field, conv_weight, qkv_weight, out_weight):
    lines = to_lines(padded_columns(field))
    planes, length, _, taps, width = lines.shape
    result = line_block(lines.reshape(length, taps * width), conv_weight, qkv_weight, out_weight)
    return to_blocks(result, field.shape[1])


def solution(mesh):
    placed = (P(None, "gx", "gy", None), P(), P(), P())
    return jax.shard_map(
        on_device, mesh=mesh, in_specs=placed, out_specs=P(None, "gx", "gy", None), check_vma=False
    )
```

```python
import jax
import jax.numpy as jnp
from jax import lax
from jax.experimental import pallas as pl
from jax.experimental.pallas import tpu as pltpu
from jax.sharding import PartitionSpec as P

HEADS = 4
HEAD = 32


def padded_columns(block):
    count = lax.axis_size("gy")
    rims = lax.optimization_barrier(block)
    left = lax.ppermute(rims[:, :, -1:], "gy", [(i, (i + 1) % count) for i in range(count)])
    right = lax.ppermute(rims[:, :, :1], "gy", [((i + 1) % count, i) for i in range(count)])
    return jnp.concatenate([left, block, right], axis=2)


def to_lines(padded):
    cols = padded.shape[2] - 2
    windows = jnp.stack([padded[:, :, b : b + cols] for b in range(3)], axis=3)
    return lax.all_to_all(windows, "gx", split_axis=2, concat_axis=1, tiled=True)


def to_blocks(result, rows):
    length, width = result.shape
    chunks = result.reshape(length // rows, rows, 1, width)
    return lax.all_to_all(chunks, "gx", split_axis=0, concat_axis=2, tiled=True)


def line_kernel(x_ref, cw_ref, qw_ref, ow_ref, o_ref):
    length = x_ref.shape[0]
    width = o_ref.shape[1]
    x = x_ref[...]
    taps = jnp.dot(x, jnp.concatenate([cw_ref[a] for a in range(3)], axis=1),
                   preferred_element_type=jnp.float32)
    stem = (taps[:, width:2 * width] + pltpu.roll(taps[:, :width], 1, 0)
            + pltpu.roll(taps[:, 2 * width:], length - 1, 0))
    mean = jnp.mean(stem, axis=-1, keepdims=True)
    centred = stem - mean
    varia = jnp.mean(centred * centred, axis=-1, keepdims=True)
    normed = (centred / jnp.sqrt(varia + 1e-05)).astype(jnp.bfloat16)
    qkv = jnp.dot(normed, qw_ref[...], preferred_element_type=jnp.float32).astype(jnp.bfloat16)
    query, keyed, valued = qkv[:, :width], qkv[:, width:2 * width], qkv[:, 2 * width:]
    head_of = lax.broadcasted_iota(jnp.int32, (length, width), 1) // HEAD
    zero = jnp.zeros_like(keyed)
    keys = jnp.concatenate([jnp.where(head_of == h, keyed, zero) for h in range(HEADS)], axis=0)
    values = jnp.concatenate([jnp.where(head_of == h, valued, zero) for h in range(HEADS)], axis=0)
    scores = lax.dot_general(query, keys, (((1,), (1,)), ((), ())), preferred_element_type=jnp.float32)
    scale = 1.0 / jnp.sqrt(jnp.float32(HEAD))
    weights, inverse = [], jnp.zeros((length, width), jnp.float32)
    for h in range(HEADS):
        s = scores[:, h * length:(h + 1) * length] * scale
        e = jnp.exp(s - jnp.max(s, axis=1, keepdims=True))
        weights.append(e.astype(jnp.bfloat16))
        inverse = jnp.where(head_of == h, 1.0 / jnp.sum(e, axis=1, keepdims=True), inverse)
    mixed = jnp.dot(jnp.concatenate(weights, axis=1), values, preferred_element_type=jnp.float32)
    attended = (mixed * inverse).astype(jnp.bfloat16)
    total = stem + jnp.dot(attended, ow_ref[...], preferred_element_type=jnp.float32)
    o_ref[...] = total.astype(o_ref.dtype)


def line_block(lines, conv_weight, qkv_weight, out_weight):
    length = lines.shape[0]; width = out_weight.shape[1]
    cw = conv_weight.reshape(3, 3 * width, width)
    vm = pl.BlockSpec(memory_space=pltpu.VMEM)
    return pl.pallas_call(line_kernel, out_shape=jax.ShapeDtypeStruct((length, width), jnp.bfloat16),
        in_specs=[vm]*4, out_specs=vm)(lines, cw, qkv_weight, out_weight)


def on_device(field, conv_weight, qkv_weight, out_weight):
    lines = to_lines(padded_columns(field))
    planes, length, _, taps, width = lines.shape
    result = line_block(lines.reshape(length, taps * width), conv_weight, qkv_weight, out_weight)
    return to_blocks(result, field.shape[1])


def solution(mesh):
    placed = (P(None, "gx", "gy", None), P(), P(), P())
    return jax.shard_map(
        on_device, mesh=mesh, in_specs=placed, out_specs=P(None, "gx", "gy", None), check_vma=False
    )
```

```python
import jax
import jax.numpy as jnp
from jax import lax
from jax.experimental import pallas as pl
from jax.experimental.pallas import tpu as pltpu
from jax.sharding import PartitionSpec as P

HEADS = 4
HEAD = 32


def to_lines(block, odd):
    planes, rows, cols, width = block.shape
    zero = jnp.zeros_like(block[:, :, :1])
    padded = jnp.concatenate([zero, block, zero], axis=2)
    windows = jnp.stack([padded[:, :, b : b + cols] for b in range(3)], axis=3)
    windows = jnp.where(odd, windows[:, :, ::-1], windows)
    lines = lax.all_to_all(windows, "gx", split_axis=2, concat_axis=1, tiled=True)
    return lines.reshape(rows * lax.axis_size("gx"), 3 * width)


def edge_lines(own):
    n_gx, n_gy = lax.axis_size("gx"), lax.axis_size("gy")
    last = n_gx - 1

    def device(j, g):
        return j * n_gy + g % n_gy

    def edge(g, first):
        return 0 if (g % 2 == 0) == first else last

    rightward = [(device(edge(g, False), g), device(edge(g, False), g + 1)) for g in range(n_gy)]
    leftward = [(device(edge(g, True), g), device(edge(g, True), g - 1)) for g in range(n_gy)]
    from_left = lax.ppermute(own, ("gx", "gy"), rightward)
    from_right = lax.ppermute(own, ("gx", "gy"), leftward)
    return from_left, from_right


def to_blocks(result, rows, odd):
    length, width = result.shape
    chunks = result.reshape(length // rows, rows, 1, width)
    block = lax.all_to_all(chunks, "gx", split_axis=0, concat_axis=2, tiled=True)
    return jnp.where(odd, block[:, :, ::-1], block)


def line_kernel(x_ref, cw_ref, qw_ref, ow_ref, o_ref):
    length = x_ref.shape[0]
    width = o_ref.shape[1]
    x = x_ref[...]
    taps = jnp.dot(x, jnp.concatenate([cw_ref[a] for a in range(3)], axis=1),
                   preferred_element_type=jnp.float32)
    stem = (taps[:, width:2 * width] + pltpu.roll(taps[:, :width], 1, 0)
            + pltpu.roll(taps[:, 2 * width:], length - 1, 0))
    mean = jnp.mean(stem, axis=-1, keepdims=True)
    centred = stem - mean
    varia = jnp.mean(centred * centred, axis=-1, keepdims=True)
    normed = (centred / jnp.sqrt(varia + 1e-05)).astype(jnp.bfloat16)
    qkv = jnp.dot(normed, qw_ref[...], preferred_element_type=jnp.float32).astype(jnp.bfloat16)
    query, keyed, valued = qkv[:, :width], qkv[:, width:2 * width], qkv[:, 2 * width:]
    head_of = lax.broadcasted_iota(jnp.int32, (length, width), 1) // HEAD
    zero = jnp.zeros_like(keyed)
    keys = jnp.concatenate([jnp.where(head_of == h, keyed, zero) for h in range(HEADS)], axis=0)
    values = jnp.concatenate([jnp.where(head_of == h, valued, zero) for h in range(HEADS)], axis=0)
    scores = lax.dot_general(query, keys, (((1,), (1,)), ((), ())), preferred_element_type=jnp.float32)
    scale = 1.0 / jnp.sqrt(jnp.float32(HEAD))
    weights, inverse = [], jnp.zeros((length, width), jnp.float32)
    for h in range(HEADS):
        s = scores[:, h * length:(h + 1) * length] * scale
        e = jnp.exp(s - jnp.max(s, axis=1, keepdims=True))
        weights.append(e.astype(jnp.bfloat16))
        inverse = jnp.where(head_of == h, 1.0 / jnp.sum(e, axis=1, keepdims=True), inverse)
    mixed = jnp.dot(jnp.concatenate(weights, axis=1), values, preferred_element_type=jnp.float32)
    attended = (mixed * inverse).astype(jnp.bfloat16)
    total = stem + jnp.dot(attended, ow_ref[...], preferred_element_type=jnp.float32)
    o_ref[...] = total.astype(o_ref.dtype)


def line_block(lines, conv_weight, qkv_weight, out_weight):
    length = lines.shape[0]; width = out_weight.shape[1]
    cw = conv_weight.reshape(3, 3 * width, width)
    vm = pl.BlockSpec(memory_space=pltpu.VMEM)
    return pl.pallas_call(line_kernel, out_shape=jax.ShapeDtypeStruct((length, width), jnp.bfloat16),
        in_specs=[vm]*4, out_specs=vm)(lines, cw, qkv_weight, out_weight)


def on_device(field, conv_weight, qkv_weight, out_weight):
    odd = lax.axis_index("gy") % 2 == 1
    width = field.shape[3]
    lines = to_lines(field, odd)
    from_left, from_right = edge_lines(lines[:, width : 2 * width])
    lines = lines + jnp.concatenate([from_left, jnp.zeros_like(from_left), from_right], axis=1)
    result = line_block(lines, conv_weight, qkv_weight, out_weight)
    return to_blocks(result, field.shape[1], odd)


def solution(mesh):
    placed = (P(None, "gx", "gy", None), P(), P(), P())
    return jax.shard_map(
        on_device, mesh=mesh, in_specs=placed, out_specs=P(None, "gx", "gy", None), check_vma=False
    )
```

```python
import jax
import jax.numpy as jnp
from jax import lax
from jax.experimental import pallas as pl
from jax.experimental.pallas import tpu as pltpu
from jax.sharding import PartitionSpec as P

HEADS = 4
HEAD = 32


def padded_columns(block):
    count = lax.axis_size("gy")
    rims = lax.optimization_barrier(block)
    tile = min(8, block.shape[2])
    left = lax.ppermute(rims[:, :, -tile:], "gy", [(i, (i + 1) % count) for i in range(count)])
    right = lax.ppermute(rims[:, :, :tile], "gy", [((i + 1) % count, i) for i in range(count)])
    return jnp.concatenate([left[:, :, -1:], block, right[:, :, :1]], axis=2)


def to_lines(padded):
    cols = padded.shape[2] - 2
    windows = jnp.stack([padded[:, :, b : b + cols] for b in range(3)], axis=3)
    return lax.all_to_all(windows, "gx", split_axis=2, concat_axis=1, tiled=True)


def to_blocks(result, rows):
    length, width = result.shape
    chunks = result.reshape(length // rows, rows, 1, width)
    return lax.all_to_all(chunks, "gx", split_axis=0, concat_axis=2, tiled=True)


def line_kernel(x_ref, cw_ref, qw_ref, ow_ref, o_ref):
    length = x_ref.shape[0]
    width = o_ref.shape[1]
    x = x_ref[...]
    taps = jnp.dot(x, jnp.concatenate([cw_ref[a] for a in range(3)], axis=1),
                   preferred_element_type=jnp.float32)
    stem = (taps[:, width:2 * width] + pltpu.roll(taps[:, :width], 1, 0)
            + pltpu.roll(taps[:, 2 * width:], length - 1, 0))
    mean = jnp.mean(stem, axis=-1, keepdims=True)
    centred = stem - mean
    varia = jnp.mean(centred * centred, axis=-1, keepdims=True)
    normed = (centred / jnp.sqrt(varia + 1e-05)).astype(jnp.bfloat16)
    qkv = jnp.dot(normed, qw_ref[...], preferred_element_type=jnp.float32).astype(jnp.bfloat16)
    query, keyed, valued = qkv[:, :width], qkv[:, width:2 * width], qkv[:, 2 * width:]
    head_of = lax.broadcasted_iota(jnp.int32, (length, width), 1) // HEAD
    zero = jnp.zeros_like(keyed)
    keys = jnp.concatenate([jnp.where(head_of == h, keyed, zero) for h in range(HEADS)], axis=0)
    values = jnp.concatenate([jnp.where(head_of == h, valued, zero) for h in range(HEADS)], axis=0)
    scores = lax.dot_general(query, keys, (((1,), (1,)), ((), ())), preferred_element_type=jnp.float32)
    scale = 1.0 / jnp.sqrt(jnp.float32(HEAD))
    weights, inverse = [], jnp.zeros((length, width), jnp.float32)
    for h in range(HEADS):
        s = scores[:, h * length:(h + 1) * length] * scale
        e = jnp.exp(s - jnp.max(s, axis=1, keepdims=True))
        weights.append(e.astype(jnp.bfloat16))
        inverse = jnp.where(head_of == h, 1.0 / jnp.sum(e, axis=1, keepdims=True), inverse)
    mixed = jnp.dot(jnp.concatenate(weights, axis=1), values, preferred_element_type=jnp.float32)
    attended = (mixed * inverse).astype(jnp.bfloat16)
    total = stem + jnp.dot(attended, ow_ref[...], preferred_element_type=jnp.float32)
    o_ref[...] = total.astype(o_ref.dtype)


def line_block(lines, conv_weight, qkv_weight, out_weight):
    length = lines.shape[0]; width = out_weight.shape[1]
    cw = conv_weight.reshape(3, 3 * width, width)
    vm = pl.BlockSpec(memory_space=pltpu.VMEM)
    return pl.pallas_call(line_kernel, out_shape=jax.ShapeDtypeStruct((length, width), jnp.bfloat16),
        in_specs=[vm]*4, out_specs=vm)(lines, cw, qkv_weight, out_weight)


def on_device(field, conv_weight, qkv_weight, out_weight):
    lines = to_lines(padded_columns(field))
    planes, length, _, taps, width = lines.shape
    result = line_block(lines.reshape(length, taps * width), conv_weight, qkv_weight, out_weight)
    return to_blocks(result, field.shape[1])


def solution(mesh):
    placed = (P(None, "gx", "gy", None), P(), P(), P())
    return jax.shard_map(
        on_device, mesh=mesh, in_specs=placed, out_specs=P(None, "gx", "gy", None), check_vma=False
    )
```

```python
import jax
import jax.numpy as jnp
from jax import lax
from jax.experimental import pallas as pl
from jax.experimental.pallas import tpu as pltpu
from jax.sharding import PartitionSpec as P

HEADS = 4
HEAD = 32


def padded_columns(block):
    count = lax.axis_size("gy")
    me = lax.axis_index("gy")
    peer = lax.broadcasted_iota(jnp.int32, (count, 1, 1, 1), 0)
    last, first = block[0, :, -1:], block[0, :, :1]
    chunks = jnp.where(peer == (me + 1) % count, last, jnp.where(peer == (me + count - 1) % count, first, 0))
    got = lax.all_to_all(chunks.astype(block.dtype), "gy", split_axis=0, concat_axis=0, tiled=True)
    left = lax.dynamic_index_in_dim(got, (me + count - 1) % count, 0, keepdims=True)
    right = lax.dynamic_index_in_dim(got, (me + 1) % count, 0, keepdims=True)
    return jnp.concatenate([left, block, right], axis=2)


def to_lines(padded):
    cols = padded.shape[2] - 2
    windows = jnp.stack([padded[:, :, b : b + cols] for b in range(3)], axis=3)
    return lax.all_to_all(windows, "gx", split_axis=2, concat_axis=1, tiled=True)


def to_blocks(result, rows):
    length, width = result.shape
    chunks = result.reshape(length // rows, rows, 1, width)
    return lax.all_to_all(chunks, "gx", split_axis=0, concat_axis=2, tiled=True)


def line_kernel(x_ref, cw_ref, qw_ref, ow_ref, o_ref):
    length = x_ref.shape[0]
    width = o_ref.shape[1]
    x = x_ref[...]
    taps = jnp.dot(x, jnp.concatenate([cw_ref[a] for a in range(3)], axis=1),
                   preferred_element_type=jnp.float32)
    stem = (taps[:, width:2 * width] + pltpu.roll(taps[:, :width], 1, 0)
            + pltpu.roll(taps[:, 2 * width:], length - 1, 0))
    mean = jnp.mean(stem, axis=-1, keepdims=True)
    centred = stem - mean
    varia = jnp.mean(centred * centred, axis=-1, keepdims=True)
    normed = (centred / jnp.sqrt(varia + 1e-05)).astype(jnp.bfloat16)
    qkv = jnp.dot(normed, qw_ref[...], preferred_element_type=jnp.float32).astype(jnp.bfloat16)
    query, keyed, valued = qkv[:, :width], qkv[:, width:2 * width], qkv[:, 2 * width:]
    head_of = lax.broadcasted_iota(jnp.int32, (length, width), 1) // HEAD
    zero = jnp.zeros_like(keyed)
    keys = jnp.concatenate([jnp.where(head_of == h, keyed, zero) for h in range(HEADS)], axis=0)
    values = jnp.concatenate([jnp.where(head_of == h, valued, zero) for h in range(HEADS)], axis=0)
    scores = lax.dot_general(query, keys, (((1,), (1,)), ((), ())), preferred_element_type=jnp.float32)
    scale = 1.0 / jnp.sqrt(jnp.float32(HEAD))
    weights, inverse = [], jnp.zeros((length, width), jnp.float32)
    for h in range(HEADS):
        s = scores[:, h * length:(h + 1) * length] * scale
        e = jnp.exp(s - jnp.max(s, axis=1, keepdims=True))
        weights.append(e.astype(jnp.bfloat16))
        inverse = jnp.where(head_of == h, 1.0 / jnp.sum(e, axis=1, keepdims=True), inverse)
    mixed = jnp.dot(jnp.concatenate(weights, axis=1), values, preferred_element_type=jnp.float32)
    attended = (mixed * inverse).astype(jnp.bfloat16)
    total = stem + jnp.dot(attended, ow_ref[...], preferred_element_type=jnp.float32)
    o_ref[...] = total.astype(o_ref.dtype)


def line_block(lines, conv_weight, qkv_weight, out_weight):
    length = lines.shape[0]; width = out_weight.shape[1]
    cw = conv_weight.reshape(3, 3 * width, width)
    vm = pl.BlockSpec(memory_space=pltpu.VMEM)
    return pl.pallas_call(line_kernel, out_shape=jax.ShapeDtypeStruct((length, width), jnp.bfloat16),
        in_specs=[vm]*4, out_specs=vm)(lines, cw, qkv_weight, out_weight)


def on_device(field, conv_weight, qkv_weight, out_weight):
    lines = to_lines(padded_columns(field))
    planes, length, _, taps, width = lines.shape
    result = line_block(lines.reshape(length, taps * width), conv_weight, qkv_weight, out_weight)
    return to_blocks(result, field.shape[1])


def solution(mesh):
    placed = (P(None, "gx", "gy", None), P(), P(), P())
    return jax.shard_map(
        on_device, mesh=mesh, in_specs=placed, out_specs=P(None, "gx", "gy", None), check_vma=False
    )
```

```python
import jax
import jax.numpy as jnp
from jax import lax
from jax.experimental import pallas as pl
from jax.experimental.pallas import tpu as pltpu
from jax.sharding import PartitionSpec as P

HEADS = 4
HEAD = 32
BLOCKS = 2


def padded_columns(block):
    count = lax.axis_size("gy")
    left = lax.ppermute(block[:, :, -1:], "gy", [(i, (i + 1) % count) for i in range(count)])
    right = lax.ppermute(block[:, :, :1], "gy", [((i + 1) % count, i) for i in range(count)])
    return jnp.concatenate([left, block, right], axis=2)


def to_lines(padded):
    cols = padded.shape[2] - 2
    windows = jnp.stack([padded[:, :, b : b + cols] for b in range(3)], axis=3)
    return lax.all_to_all(windows, "gx", split_axis=2, concat_axis=1, tiled=True)


def to_blocks(result, rows):
    length, width = result.shape
    chunks = result.reshape(length // rows, rows, 1, width)
    return lax.all_to_all(chunks, "gx", split_axis=0, concat_axis=2, tiled=True)


def line_kernel(x_ref, cw_ref, qw_ref, ow_ref, o_ref):
    length = x_ref.shape[0]
    width = o_ref.shape[1]
    x = x_ref[...]
    taps = jnp.dot(x, jnp.concatenate([cw_ref[a] for a in range(3)], axis=1),
                   preferred_element_type=jnp.float32)
    stem = (taps[:, width:2 * width] + pltpu.roll(taps[:, :width], 1, 0)
            + pltpu.roll(taps[:, 2 * width:], length - 1, 0))
    mean = jnp.mean(stem, axis=-1, keepdims=True)
    centred = stem - mean
    varia = jnp.mean(centred * centred, axis=-1, keepdims=True)
    normed = (centred / jnp.sqrt(varia + 1e-05)).astype(jnp.bfloat16)
    qkv = jnp.dot(normed, qw_ref[...], preferred_element_type=jnp.float32).astype(jnp.bfloat16)
    query, keyed, valued = qkv[:, :width], qkv[:, width:2 * width], qkv[:, 2 * width:]
    head_of = lax.broadcasted_iota(jnp.int32, (length, width), 1) // HEAD
    zero = jnp.zeros_like(keyed)
    keys = jnp.concatenate([jnp.where(head_of == h, keyed, zero) for h in range(HEADS)], axis=0)
    values = jnp.concatenate([jnp.where(head_of == h, valued, zero) for h in range(HEADS)], axis=0)
    scale = 1.0 / jnp.sqrt(jnp.float32(HEAD))
    rows = length // BLOCKS
    parts = []
    for r in range(BLOCKS):
        part = slice(r * rows, (r + 1) * rows)
        scores = lax.dot_general(query[part], keys, (((1,), (1,)), ((), ())),
                                 preferred_element_type=jnp.float32)
        weights, inverse = [], jnp.zeros((rows, width), jnp.float32)
        for h in range(HEADS):
            s = scores[:, h * length:(h + 1) * length] * scale
            e = jnp.exp(s - jnp.max(s, axis=1, keepdims=True))
            weights.append(e.astype(jnp.bfloat16))
            inverse = jnp.where(head_of[part] == h, 1.0 / jnp.sum(e, axis=1, keepdims=True), inverse)
        mixed = jnp.dot(jnp.concatenate(weights, axis=1), values, preferred_element_type=jnp.float32)
        parts.append((mixed * inverse).astype(jnp.bfloat16))
    attended = jnp.concatenate(parts, axis=0)
    total = stem + jnp.dot(attended, ow_ref[...], preferred_element_type=jnp.float32)
    o_ref[...] = total.astype(o_ref.dtype)


def line_block(lines, conv_weight, qkv_weight, out_weight):
    length = lines.shape[0]; width = out_weight.shape[1]
    cw = conv_weight.reshape(3, 3 * width, width)
    vm = pl.BlockSpec(memory_space=pltpu.VMEM)
    return pl.pallas_call(line_kernel, out_shape=jax.ShapeDtypeStruct((length, width), jnp.bfloat16),
        in_specs=[vm]*4, out_specs=vm)(lines, cw, qkv_weight, out_weight)


def on_device(field, conv_weight, qkv_weight, out_weight):
    lines = to_lines(padded_columns(field))
    planes, length, _, taps, width = lines.shape
    result = line_block(lines.reshape(length, taps * width), conv_weight, qkv_weight, out_weight)
    return to_blocks(result, field.shape[1])


def solution(mesh):
    placed = (P(None, "gx", "gy", None), P(), P(), P())
    return jax.shard_map(
        on_device, mesh=mesh, in_specs=placed, out_specs=P(None, "gx", "gy", None), check_vma=False
    )
```

```python
import jax
import jax.numpy as jnp
from jax import lax
from jax.experimental import pallas as pl
from jax.experimental.pallas import tpu as pltpu
from jax.sharding import PartitionSpec as P

HEADS = 4
HEAD = 32
BLOCKS = 2


def padded_columns(block):
    count = lax.axis_size("gy")
    left = lax.ppermute(block[:, :, -1:], "gy", [(i, (i + 1) % count) for i in range(count)])
    right = lax.ppermute(block[:, :, :1], "gy", [((i + 1) % count, i) for i in range(count)])
    return jnp.concatenate([left, block, right], axis=2)


def to_lines(padded):
    cols = padded.shape[2] - 2
    windows = jnp.stack([padded[:, :, b : b + cols] for b in range(3)], axis=3)
    return lax.all_to_all(windows, "gx", split_axis=2, concat_axis=1, tiled=True)


def to_blocks(result, rows):
    length, width = result.shape
    chunks = result.reshape(length // rows, rows, 1, width)
    return lax.all_to_all(chunks, "gx", split_axis=0, concat_axis=2, tiled=True)


def line_kernel(x_ref, cw_ref, qw_ref, ow_ref, o_ref):
    length = x_ref.shape[0]
    width = o_ref.shape[1]
    rows = length // BLOCKS
    x = x_ref[...]
    taps = jnp.dot(x, jnp.concatenate([cw_ref[a] for a in range(3)], axis=1),
                   preferred_element_type=jnp.float32)
    stem = (taps[:, width:2 * width] + pltpu.roll(taps[:, :width], 1, 0)
            + pltpu.roll(taps[:, 2 * width:], length - 1, 0))
    halves = [slice(r * rows, (r + 1) * rows) for r in range(BLOCKS)]
    qkvs = []
    for part in halves:
        piece = stem[part]
        mean = jnp.mean(piece, axis=-1, keepdims=True)
        centred = piece - mean
        varia = jnp.mean(centred * centred, axis=-1, keepdims=True)
        normed = (centred / jnp.sqrt(varia + 1e-05)).astype(jnp.bfloat16)
        qkvs.append(jnp.dot(normed, qw_ref[...], preferred_element_type=jnp.float32).astype(jnp.bfloat16))
    qkv = jnp.concatenate(qkvs, axis=0)
    keyed, valued = qkv[:, width:2 * width], qkv[:, 2 * width:]
    head_of = lax.broadcasted_iota(jnp.int32, (length, width), 1) // HEAD
    zero = jnp.zeros_like(keyed)
    keys = jnp.concatenate([jnp.where(head_of == h, keyed, zero) for h in range(HEADS)], axis=0)
    values = jnp.concatenate([jnp.where(head_of == h, valued, zero) for h in range(HEADS)], axis=0)
    scale = 1.0 / jnp.sqrt(jnp.float32(HEAD))
    for r, part in enumerate(halves):
        scores = lax.dot_general(qkvs[r][:, :width], keys, (((1,), (1,)), ((), ())),
                                 preferred_element_type=jnp.float32)
        weights, inverse = [], jnp.zeros((rows, width), jnp.float32)
        for h in range(HEADS):
            s = scores[:, h * length:(h + 1) * length] * scale
            e = jnp.exp(s - jnp.max(s, axis=1, keepdims=True))
            weights.append(e.astype(jnp.bfloat16))
            inverse = jnp.where(head_of[part] == h, 1.0 / jnp.sum(e, axis=1, keepdims=True), inverse)
        mixed = jnp.dot(jnp.concatenate(weights, axis=1), values, preferred_element_type=jnp.float32)
        attended = (mixed * inverse).astype(jnp.bfloat16)
        total = stem[part] + jnp.dot(attended, ow_ref[...], preferred_element_type=jnp.float32)
        o_ref[part, :] = total.astype(o_ref.dtype)


def line_block(lines, conv_weight, qkv_weight, out_weight):
    length = lines.shape[0]; width = out_weight.shape[1]
    cw = conv_weight.reshape(3, 3 * width, width)
    vm = pl.BlockSpec(memory_space=pltpu.VMEM)
    return pl.pallas_call(line_kernel, out_shape=jax.ShapeDtypeStruct((length, width), jnp.bfloat16),
        in_specs=[vm]*4, out_specs=vm)(lines, cw, qkv_weight, out_weight)


def on_device(field, conv_weight, qkv_weight, out_weight):
    lines = to_lines(padded_columns(field))
    planes, length, _, taps, width = lines.shape
    result = line_block(lines.reshape(length, taps * width), conv_weight, qkv_weight, out_weight)
    return to_blocks(result, field.shape[1])


def solution(mesh):
    placed = (P(None, "gx", "gy", None), P(), P(), P())
    return jax.shard_map(
        on_device, mesh=mesh, in_specs=placed, out_specs=P(None, "gx", "gy", None), check_vma=False
    )
```

```python
import jax
import jax.numpy as jnp
from jax import lax
from jax.experimental import pallas as pl
from jax.experimental.pallas import tpu as pltpu
from jax.sharding import PartitionSpec as P

HEADS = 4
HEAD = 32
BLOCKS = 2


def padded_columns(block):
    count = lax.axis_size("gy")
    left = lax.ppermute(block[:, :, -1:], "gy", [(i, (i + 1) % count) for i in range(count)])
    right = lax.ppermute(block[:, :, :1], "gy", [((i + 1) % count, i) for i in range(count)])
    return jnp.concatenate([left, block, right], axis=2)


def to_lines(padded):
    cols = padded.shape[2] - 2
    windows = jnp.stack([padded[:, :, b : b + cols] for b in range(3)], axis=3)
    return lax.all_to_all(windows, "gx", split_axis=2, concat_axis=1, tiled=True)


def to_blocks(result, rows):
    length, width = result.shape
    chunks = result.reshape(length // rows, rows, 1, width)
    return lax.all_to_all(chunks, "gx", split_axis=0, concat_axis=2, tiled=True)


def line_kernel(x_ref, cw_ref, qw_ref, ow_ref, o_ref):
    length = x_ref.shape[0]
    width = o_ref.shape[1]
    x = x_ref[...]
    taps = jnp.dot(x, jnp.concatenate([cw_ref[a] for a in range(3)], axis=1),
                   preferred_element_type=jnp.float32)
    stem = (taps[:, width:2 * width] + pltpu.roll(taps[:, :width], 1, 0)
            + pltpu.roll(taps[:, 2 * width:], length - 1, 0))
    mean = jnp.mean(stem, axis=-1, keepdims=True)
    centred = stem - mean
    varia = jnp.mean(centred * centred, axis=-1, keepdims=True)
    normed = (centred / jnp.sqrt(varia + 1e-05)).astype(jnp.bfloat16)
    qkv = jnp.dot(normed, qw_ref[...], preferred_element_type=jnp.float32).astype(jnp.bfloat16)
    query, keyed, valued = qkv[:, :width], qkv[:, width:2 * width], qkv[:, 2 * width:]
    head_of = lax.broadcasted_iota(jnp.int32, (length, width), 1) // HEAD
    zero = jnp.zeros_like(keyed)
    keys = jnp.concatenate([jnp.where(head_of == h, keyed, zero) for h in range(HEADS)], axis=0)
    values = jnp.concatenate([jnp.where(head_of == h, valued, zero) for h in range(HEADS)], axis=0)
    scale = 1.0 / jnp.sqrt(jnp.float32(HEAD))
    rows = length // BLOCKS
    for r in range(BLOCKS):
        part = slice(r * rows, (r + 1) * rows)
        scores = lax.dot_general(query[part], keys, (((1,), (1,)), ((), ())),
                                 preferred_element_type=jnp.float32)
        weights, inverse = [], jnp.zeros((rows, width), jnp.float32)
        for h in range(HEADS):
            s = scores[:, h * length:(h + 1) * length] * scale
            e = jnp.exp(s - jnp.max(s, axis=1, keepdims=True))
            weights.append(e.astype(jnp.bfloat16))
            inverse = jnp.where(head_of[part] == h, 1.0 / jnp.sum(e, axis=1, keepdims=True), inverse)
        mixed = jnp.dot(jnp.concatenate(weights, axis=1), values, preferred_element_type=jnp.float32)
        attended = (mixed * inverse).astype(jnp.bfloat16)
        total = stem[part] + jnp.dot(attended, ow_ref[...], preferred_element_type=jnp.float32)
        o_ref[part, :] = total.astype(o_ref.dtype)


def line_block(lines, conv_weight, qkv_weight, out_weight):
    length = lines.shape[0]; width = out_weight.shape[1]
    cw = conv_weight.reshape(3, 3 * width, width)
    vm = pl.BlockSpec(memory_space=pltpu.VMEM)
    return pl.pallas_call(line_kernel, out_shape=jax.ShapeDtypeStruct((length, width), jnp.bfloat16),
        in_specs=[vm]*4, out_specs=vm)(lines, cw, qkv_weight, out_weight)


def on_device(field, conv_weight, qkv_weight, out_weight):
    lines = to_lines(padded_columns(field))
    planes, length, _, taps, width = lines.shape
    result = line_block(lines.reshape(length, taps * width), conv_weight, qkv_weight, out_weight)
    return to_blocks(result, field.shape[1])


def solution(mesh):
    placed = (P(None, "gx", "gy", None), P(), P(), P())
    return jax.shard_map(
        on_device, mesh=mesh, in_specs=placed, out_specs=P(None, "gx", "gy", None), check_vma=False
    )
```

```python
import jax
import jax.numpy as jnp
from jax import lax
from jax.experimental import pallas as pl
from jax.experimental.pallas import tpu as pltpu
from jax.sharding import PartitionSpec as P

HEADS = 4
HEAD = 32
BLOCKS = 2


def swap_kernel(x_ref, o_ref):
    o_ref[...] = jnp.swapaxes(x_ref[...].astype(jnp.float32), 0, 1).astype(o_ref.dtype)


def column_major(block):
    rows, cols, width = block.shape
    vm = pl.BlockSpec(memory_space=pltpu.VMEM)
    return pl.pallas_call(swap_kernel, out_shape=jax.ShapeDtypeStruct((cols, rows, width), block.dtype),
        in_specs=[vm], out_specs=vm)(block)


def padded_columns(block):
    count = lax.axis_size("gy")
    columns = column_major(block[0])
    left = lax.ppermute(columns[-1:], "gy", [(i, (i + 1) % count) for i in range(count)])
    right = lax.ppermute(columns[:1], "gy", [((i + 1) % count, i) for i in range(count)])
    return jnp.concatenate([left, columns, right], axis=0)


def to_lines(padded):
    cols, rows, width = padded.shape[0] - 2, padded.shape[1], padded.shape[2]
    windows = jnp.stack([padded[b : b + cols] for b in range(3)], axis=2)
    lines = lax.all_to_all(windows, "gx", split_axis=0, concat_axis=0, tiled=True)
    return lines.reshape(cols * rows, 3 * width)


def to_blocks(result, rows):
    length, width = result.shape
    chunks = result.reshape(length // rows, rows, 1, width)
    return lax.all_to_all(chunks, "gx", split_axis=0, concat_axis=2, tiled=True)


def line_kernel(x_ref, cw_ref, qw_ref, ow_ref, o_ref):
    length = x_ref.shape[0]
    width = o_ref.shape[1]
    x = x_ref[...]
    taps = jnp.dot(x, jnp.concatenate([cw_ref[a] for a in range(3)], axis=1),
                   preferred_element_type=jnp.float32)
    stem = (taps[:, width:2 * width] + pltpu.roll(taps[:, :width], 1, 0)
            + pltpu.roll(taps[:, 2 * width:], length - 1, 0))
    mean = jnp.mean(stem, axis=-1, keepdims=True)
    centred = stem - mean
    varia = jnp.mean(centred * centred, axis=-1, keepdims=True)
    normed = (centred / jnp.sqrt(varia + 1e-05)).astype(jnp.bfloat16)
    qkv = jnp.dot(normed, qw_ref[...], preferred_element_type=jnp.float32).astype(jnp.bfloat16)
    query, keyed, valued = qkv[:, :width], qkv[:, width:2 * width], qkv[:, 2 * width:]
    head_of = lax.broadcasted_iota(jnp.int32, (length, width), 1) // HEAD
    zero = jnp.zeros_like(keyed)
    keys = jnp.concatenate([jnp.where(head_of == h, keyed, zero) for h in range(HEADS)], axis=0)
    values = jnp.concatenate([jnp.where(head_of == h, valued, zero) for h in range(HEADS)], axis=0)
    scale = 1.0 / jnp.sqrt(jnp.float32(HEAD))
    rows = length // BLOCKS
    parts = []
    for r in range(BLOCKS):
        part = slice(r * rows, (r + 1) * rows)
        scores = lax.dot_general(query[part], keys, (((1,), (1,)), ((), ())),
                                 preferred_element_type=jnp.float32)
        weights, inverse = [], jnp.zeros((rows, width), jnp.float32)
        for h in range(HEADS):
            s = scores[:, h * length:(h + 1) * length] * scale
            e = jnp.exp(s - jnp.max(s, axis=1, keepdims=True))
            weights.append(e.astype(jnp.bfloat16))
            inverse = jnp.where(head_of[part] == h, 1.0 / jnp.sum(e, axis=1, keepdims=True), inverse)
        mixed = jnp.dot(jnp.concatenate(weights, axis=1), values, preferred_element_type=jnp.float32)
        parts.append((mixed * inverse).astype(jnp.bfloat16))
    attended = jnp.concatenate(parts, axis=0)
    total = stem + jnp.dot(attended, ow_ref[...], preferred_element_type=jnp.float32)
    o_ref[...] = total.astype(o_ref.dtype)


def line_block(lines, conv_weight, qkv_weight, out_weight):
    length = lines.shape[0]; width = out_weight.shape[1]
    cw = conv_weight.reshape(3, 3 * width, width)
    vm = pl.BlockSpec(memory_space=pltpu.VMEM)
    return pl.pallas_call(line_kernel, out_shape=jax.ShapeDtypeStruct((length, width), jnp.bfloat16),
        in_specs=[vm]*4, out_specs=vm)(lines, cw, qkv_weight, out_weight)


def on_device(field, conv_weight, qkv_weight, out_weight):
    lines = to_lines(padded_columns(field))
    result = line_block(lines, conv_weight, qkv_weight, out_weight)
    return to_blocks(result, field.shape[1])


def solution(mesh):
    placed = (P(None, "gx", "gy", None), P(), P(), P())
    return jax.shard_map(
        on_device, mesh=mesh, in_specs=placed, out_specs=P(None, "gx", "gy", None), check_vma=False
    )
```

```python
import jax
import jax.numpy as jnp
from jax import lax
from jax.experimental import pallas as pl
from jax.experimental.pallas import tpu as pltpu
from jax.sharding import PartitionSpec as P

HEADS = 4
HEAD = 32
BLOCKS = 2


def padded_columns(block):
    count = lax.axis_size("gy")
    left = lax.ppermute(block[:, :, -1:], "gy", [(i, (i + 1) % count) for i in range(count)])
    right = lax.ppermute(block[:, :, :1], "gy", [((i + 1) % count, i) for i in range(count)])
    return jnp.concatenate([left, block, right], axis=2)


def to_lines(padded):
    cols = padded.shape[2] - 2
    windows = jnp.stack([padded[:, :, b : b + cols] for b in range(3)], axis=3)
    return lax.all_to_all(windows, "gx", split_axis=2, concat_axis=1, tiled=True)


def to_blocks(result, rows):
    length, width = result.shape
    chunks = result.reshape(length // rows, rows, 1, width)
    return lax.all_to_all(chunks, "gx", split_axis=0, concat_axis=2, tiled=True)


def line_kernel(x_ref, cw_ref, qw_ref, ow_ref, o_ref):
    length = x_ref.shape[0]
    width = o_ref.shape[1]
    x = x_ref[...]
    taps = jnp.dot(x, jnp.concatenate([cw_ref[a] for a in range(3)], axis=1),
                   preferred_element_type=jnp.float32)
    stem = (taps[:, width:2 * width] + pltpu.roll(taps[:, :width], 1, 0)
            + pltpu.roll(taps[:, 2 * width:], length - 1, 0))
    mean = jnp.mean(stem, axis=-1, keepdims=True)
    centred = stem - mean
    varia = jnp.mean(centred * centred, axis=-1, keepdims=True)
    normed = (centred / jnp.sqrt(varia + 1e-05)).astype(jnp.bfloat16)
    qkv = jnp.dot(normed, qw_ref[...], preferred_element_type=jnp.float32).astype(jnp.bfloat16)
    query, keyed, valued = qkv[:, :width], qkv[:, width:2 * width], qkv[:, 2 * width:]
    head_of = lax.broadcasted_iota(jnp.int32, (length, width), 1) // HEAD
    zero = jnp.zeros_like(keyed)
    keys = jnp.concatenate([jnp.where(head_of == h, keyed, zero) for h in range(HEADS)], axis=0)
    values = jnp.concatenate([jnp.where(head_of == h, valued, zero) for h in range(HEADS)], axis=0)
    scale = 1.0 / jnp.sqrt(jnp.float32(HEAD))
    rows = length // BLOCKS
    parts = []
    for r in range(BLOCKS):
        part = slice(r * rows, (r + 1) * rows)
        scores = lax.dot_general(query[part], keys, (((1,), (1,)), ((), ())),
                                 preferred_element_type=jnp.float32)
        weights, inverse = [], jnp.zeros((rows, width), jnp.float32)
        for h in range(HEADS):
            s = scores[:, h * length:(h + 1) * length] * scale
            e = jnp.exp(s - jnp.max(s, axis=1, keepdims=True))
            weights.append(e.astype(jnp.bfloat16))
            inverse = jnp.where(head_of[part] == h, 1.0 / jnp.sum(e, axis=1, keepdims=True), inverse)
        mixed = jnp.dot(jnp.concatenate(weights, axis=1), values, preferred_element_type=jnp.float32)
        parts.append((mixed * inverse).astype(jnp.bfloat16))
    attended = jnp.concatenate(parts, axis=0)
    total = stem + jnp.dot(attended, ow_ref[...], preferred_element_type=jnp.float32)
    o_ref[...] = total.astype(o_ref.dtype)


def line_block(lines, conv_weight, qkv_weight, out_weight):
    length = lines.shape[0]; width = out_weight.shape[1]
    cw, qw, ow = (pltpu.with_memory_space_constraint(w, pltpu.VMEM)
                  for w in (conv_weight.reshape(3, 3 * width, width), qkv_weight, out_weight))
    vm = pl.BlockSpec(memory_space=pltpu.VMEM)
    return pl.pallas_call(line_kernel, out_shape=jax.ShapeDtypeStruct((length, width), jnp.bfloat16),
        in_specs=[vm]*4, out_specs=vm)(lines, cw, qw, ow)


def on_device(field, conv_weight, qkv_weight, out_weight):
    lines = to_lines(padded_columns(field))
    planes, length, _, taps, width = lines.shape
    result = line_block(lines.reshape(length, taps * width), conv_weight, qkv_weight, out_weight)
    return to_blocks(result, field.shape[1])


def solution(mesh):
    placed = (P(None, "gx", "gy", None), P(), P(), P())
    return jax.shard_map(
        on_device, mesh=mesh, in_specs=placed, out_specs=P(None, "gx", "gy", None), check_vma=False
    )
```
